8 devices in a mesh: dp: 1 (over z), tp: 2 (over y), sp: 4 (over x, core).
Axes of the slice: x: 2, y: 2, z: 1, core: 2. Of those that a mesh axis runs over, the one named last changes fastest.
Arguments:
- tokens: bfloat16 [8192, 4096], P(('dp', 'sp'))
- glob_pos: int32 [512], P('dp')
- w_query: bfloat16 [4096, 32, 128], P(None, 'tp')
- w_key: bfloat16 [4096, 32, 128], P(None, 'tp')
- w_value: bfloat16 [4096, 32, 128], P(None, 'tp')
- w_out: bfloat16 [32, 128, 4096], P('tp')
- w_up: bfloat16 [4096, 14336], P(None, 'tp')
- w_down: bfloat16 [14336, 4096], P('tp')
Outputs:
- output: bfloat16 [8192, 4096], P(('dp', 'sp'))
All inputs are finite; a program needn't handle non-finite values.
Results may differ from the reference program's by a relative error of at most 0.0118318.
Values are sent between devices in bfloat16 or wider.
A program may use at most 1 GiB of HBM per device.

```python
import jax
import jax.numpy as jnp
from jax import lax
import math

D = 4096
HEADS = 32
FF = 14336
WIN = 256
SEQ = 8192
GLOB = 512

HEAD = D // HEADS


def setup_inputs(seed: int = 0, part: int = 0) -> dict:
    root_key = jax.random.key(seed)
    weight_root, part_root = jax.random.split(root_key, 2)
    part_key = jax.random.fold_in(part_root, part)
    tok_key, pos_key = jax.random.split(part_key, 2)
    tokens = jax.random.normal(tok_key, (SEQ, D), jnp.float32).astype(jnp.bfloat16)
    inner_pos = jax.random.permutation(pos_key, SEQ - 2)[: GLOB - 2] + 1
    glob_pos = jnp.sort(jnp.concatenate([jnp.array([0, SEQ - 1], jnp.int32), inner_pos.astype(jnp.int32)]))
    w_keys = jax.random.split(weight_root, 7)
    qk_std = (2.0 / D) ** 0.5
    out_std = max(1.0, ((2 * WIN + GLOB) / 50.0) ** 0.5) / math.sqrt(D)
    w_query = (jax.random.normal(w_keys[0], (D, HEADS, HEAD), jnp.float32) * qk_std).astype(jnp.bfloat16)
    w_key = (jax.random.normal(w_keys[1], (D, HEADS, HEAD), jnp.float32) * qk_std).astype(jnp.bfloat16)
    w_value = (jax.random.normal(w_keys[2], (D, HEADS, HEAD), jnp.float32) / math.sqrt(D)).astype(jnp.bfloat16)
    w_out = (jax.random.normal(w_keys[3], (HEADS, HEAD, D), jnp.float32) * out_std).astype(jnp.bfloat16)
    w_up = (jax.random.normal(w_keys[4], (D, FF), jnp.float32) / math.sqrt(D)).astype(jnp.bfloat16)
    w_down = (jax.random.normal(w_keys[5], (FF, D), jnp.float32) / math.sqrt(FF)).astype(jnp.bfloat16)
    return {'tokens': tokens, 'glob_pos': glob_pos, 'w_query': w_query, 'w_key': w_key, 'w_value': w_value, 'w_out': w_out, 'w_up': w_up, 'w_down': w_down}


def reference(tokens, glob_pos, w_query, w_key, w_value, w_out, w_up, w_down):
    scale = 1.0 / math.sqrt(HEAD)
    q_rows = jnp.dot(tokens, w_query.reshape(D, D), preferred_element_type=jnp.float32).astype(jnp.bfloat16).reshape(SEQ, HEADS, HEAD)
    k_rows = jnp.dot(tokens, w_key.reshape(D, D), preferred_element_type=jnp.float32).astype(jnp.bfloat16).reshape(SEQ, HEADS, HEAD)
    v_rows = jnp.dot(tokens, w_value.reshape(D, D), preferred_element_type=jnp.float32).astype(jnp.bfloat16).reshape(SEQ, HEADS, HEAD)
    glob_flag = jnp.zeros((SEQ,), jnp.int32).at[glob_pos].set(1)
    pad_cfg = ((WIN, WIN), (0, 0), (0, 0))
    k_pad = jnp.pad(k_rows, pad_cfg)
    v_pad = jnp.pad(v_rows, pad_cfg)
    flag_pad = jnp.pad(glob_flag, (WIN, WIN))
    k_glob = k_rows[glob_pos].astype(jnp.float32)
    v_glob = v_rows[glob_pos].astype(jnp.float32)
    q_block = 128
    key_span = q_block + 2 * WIN

    def window_block(blk_index):
        start = blk_index * q_block
        q_blk = lax.dynamic_slice_in_dim(q_rows, start, q_block).astype(jnp.float32)
        k_blk = lax.dynamic_slice_in_dim(k_pad, start, key_span).astype(jnp.float32)
        v_blk = lax.dynamic_slice_in_dim(v_pad, start, key_span).astype(jnp.float32)
        f_blk = lax.dynamic_slice_in_dim(flag_pad, start, key_span)
        q_pos = start + jnp.arange(q_block)
        k_pos = start - WIN + jnp.arange(key_span)
        k_ok = (k_pos >= 0) & (k_pos < SEQ) & (f_blk == 0)
        allowed = (jnp.abs(q_pos[:, None] - k_pos[None, :]) <= WIN) & k_ok[None, :]
        s_win = jnp.einsum('qhe,khe->hqk', q_blk, k_blk) * scale
        s_win = jnp.where(allowed[None], s_win, -jnp.inf)
        s_glob = jnp.einsum('qhe,ghe->hqg', q_blk, k_glob) * scale
        prob_rows = jax.nn.softmax(jnp.concatenate([s_win, s_glob], axis=2), axis=2)
        prob_rows = prob_rows.astype(jnp.bfloat16).astype(jnp.float32)
        v_all = jnp.concatenate([v_blk, v_glob], axis=0)
        return jnp.einsum('hqk,khe->qhe', prob_rows, v_all).astype(jnp.bfloat16)

    o_rows = lax.map(window_block, jnp.arange(SEQ // q_block)).reshape(SEQ, HEADS, HEAD)
    q_heads = jnp.transpose(q_rows[glob_pos], (1, 0, 2))
    k_heads = jnp.transpose(k_rows, (1, 0, 2))
    v_heads = jnp.transpose(v_rows, (1, 0, 2))

    def glob_head(head_parts):
        q_head, k_head, v_head = head_parts
        scores = jnp.dot(q_head, k_head.T, preferred_element_type=jnp.float32) * scale
        prob_rows = jax.nn.softmax(scores, axis=1).astype(jnp.bfloat16)
        return jnp.dot(prob_rows, v_head, preferred_element_type=jnp.float32).astype(jnp.bfloat16)

    glob_out = jnp.transpose(lax.map(glob_head, (q_heads, k_heads, v_heads)), (1, 0, 2))
    o_rows = o_rows.at[glob_pos].set(glob_out)
    mixed = jnp.dot(o_rows.reshape(SEQ, D), w_out.reshape(D, D), preferred_element_type=jnp.float32)
    hidden = (tokens.astype(jnp.float32) + mixed).astype(jnp.bfloat16)
    gelu_rows = jax.nn.gelu(jnp.dot(hidden, w_up, preferred_element_type=jnp.float32), approximate=True).astype(jnp.bfloat16)
    down_sum = jnp.dot(gelu_rows, w_down, preferred_element_type=jnp.float32)
    return (hidden.astype(jnp.float32) + down_sum).astype(jnp.bfloat16)
```

```python
import functools
import math

import jax
import jax.numpy as jnp
from jax import lax
from jax.experimental import pallas as pl
from jax.experimental.pallas import tpu as pltpu
from jax.sharding import PartitionSpec as P


WIN = 256
QB = 256
ROWS = 512
F32 = jnp.float32
BF16 = jnp.bfloat16
LOG2E = 1.4426950408889634


def contract_last(a, b):
    return lax.dot_general(a, b, (((1,), (1,)), ((), ())), preferred_element_type=F32)


def contract_first(a, b):
    return lax.dot_general(a, b, (((0,), (0,)), ((), ())), preferred_element_type=F32)


def window_kernel(r0_ref, q_ref, k_ref, v_ref, lk_ref, lv_ref, rk_ref, rv_ref, kg_ref, vg_ref, bias_ref, o_ref,
                  k_win, v_win, mask, *, coef):
    n_rows = k_ref.shape[1]
    r0 = pl.multiple_of(r0_ref[0], ROWS)

    @pl.when(pl.program_id(0) == 0)
    def _():
        key = lax.broadcasted_iota(jnp.int32, (QB + 2 * WIN, QB), 0)
        query = lax.broadcasted_iota(jnp.int32, (QB + 2 * WIN, QB), 1)
        band = (key >= query) & (key <= query + 2 * WIN)
        for b in range(ROWS // QB):
            rows = bias_ref[pl.ds(pl.multiple_of(r0 + b * QB, QB), QB + 2 * WIN), :]
            mask[b] = jnp.where(band, jnp.concatenate([rows] * (QB // 128), axis=1), -jnp.inf)

    before = pl.multiple_of(jnp.maximum(r0 - WIN, 0), WIN)
    after = pl.multiple_of(jnp.minimum(r0 + ROWS, n_rows - WIN), WIN)
    for src, left, right, dst in ((k_ref, lk_ref, rk_ref, k_win), (v_ref, lv_ref, rv_ref, v_win)):
        dst[0:WIN, :] = jnp.where(r0 == 0, left[0], src[0, pl.ds(before, WIN), :])
        dst[WIN:WIN + ROWS, :] = src[0, pl.ds(r0, ROWS), :]
        dst[WIN + ROWS:, :] = jnp.where(r0 + ROWS == n_rows, right[0], src[0, pl.ds(after, WIN), :])

    def scores(b):
        q_blk = q_ref[0, b * QB:(b + 1) * QB, :]
        s_win = contract_last(k_win[b * QB:(b + 1) * QB + 2 * WIN, :], q_blk) * coef + mask[b]
        return s_win, contract_last(kg_ref[0], q_blk) * coef

    s_win, s_glob = scores(0)
    for b in range(ROWS // QB):
        following = scores(b + 1) if b + 1 < ROWS // QB else (None, None)
        top = jnp.maximum(jnp.max(s_win, axis=0, keepdims=True), jnp.max(s_glob, axis=0, keepdims=True))
        e_win = jnp.exp2(s_win - top)
        e_glob = jnp.exp2(s_glob - top)
        inv = 1.0 / (jnp.sum(e_win, axis=0, keepdims=True) + jnp.sum(e_glob, axis=0, keepdims=True))
        out = contract_first(v_win[b * QB:(b + 1) * QB + 2 * WIN, :], (e_win * inv).astype(BF16))
        out = out + contract_first(vg_ref[0], (e_glob * inv).astype(BF16))
        o_ref[b * QB:(b + 1) * QB, :] = out.T.astype(BF16)
        s_win, s_glob = following


def window_rows(r0, q, k, v, left_k, left_v, right_k, right_v, k_glob, v_glob, bias):
    n_heads, n_rows, dim = q.shape
    n_glob = k_glob.shape[1]

    def head(shape):
        return pl.BlockSpec((1,) + shape, lambda h, r: (h, 0, 0))

    span = ROWS + 2 * WIN
    work = n_heads * ROWS * (QB + 2 * WIN + n_glob)
    return pl.pallas_call(
        functools.partial(window_kernel, coef=LOG2E / math.sqrt(dim)),
        out_shape=jax.ShapeDtypeStruct((ROWS, n_heads * dim), BF16),
        grid_spec=pltpu.PrefetchScalarGridSpec(
            num_scalar_prefetch=1,
            grid=(n_heads,),
            in_specs=[
                pl.BlockSpec((1, ROWS, dim), lambda h, r: (h, r[0] // ROWS, 0)),
                head((n_rows, dim)), head((n_rows, dim)),
                head((WIN, dim)), head((WIN, dim)), head((WIN, dim)), head((WIN, dim)),
                head((n_glob, dim)), head((n_glob, dim)),
                pl.BlockSpec(bias.shape, lambda h, r: (0, 0)),
            ],
            out_specs=pl.BlockSpec((ROWS, dim), lambda h, r: (0, h)),
            scratch_shapes=[
                pltpu.VMEM((span, dim), BF16),
                pltpu.VMEM((span, dim), BF16),
                pltpu.VMEM((ROWS // QB, QB + 2 * WIN, QB), F32),
            ],
        ),
        cost_estimate=pl.CostEstimate(flops=8 * work * dim, bytes_accessed=28 << 20, transcendentals=work),
        compiler_params=pltpu.CompilerParams(dimension_semantics=("arbitrary",), vmem_limit_bytes=62 << 20),
        name="window_attention",
    )(r0, q, k, v, left_k, left_v, right_k, right_v, k_glob, v_glob, bias)


def glob_kernel(q_ref, k_ref, v_ref, o_ref, *, coef):
    dim = q_ref.shape[2]
    n_blocks = q_ref.shape[1] // QB

    def scores(b):
        return contract_last(k_ref[0], q_ref[0, b * QB:(b + 1) * QB, :]) * coef

    s = scores(0)
    for b in range(n_blocks):
        following = scores(b + 1) if b + 1 < n_blocks else None
        cols = slice(b * QB, (b + 1) * QB)
        top = jnp.max(s, axis=0, keepdims=True)
        e = jnp.exp2(s - top)
        total = jnp.sum(e, axis=0, keepdims=True)
        o_ref[0, 0:dim, cols] = contract_first(v_ref[0], (e * (1.0 / total)).astype(BF16))
        row = lax.broadcasted_iota(jnp.int32, (8, QB), 0)
        o_ref[0, dim:, cols] = jnp.where(row == 0, top, total)
        s = following


def glob_part(q_glob, k, v):
    n_heads, n_glob, dim = q_glob.shape
    n_rows = k.shape[1]
    work = n_heads * n_rows * n_glob

    def head(shape):
        return pl.BlockSpec((1,) + shape, lambda h: (h, 0, 0))

    return pl.pallas_call(
        functools.partial(glob_kernel, coef=LOG2E / math.sqrt(dim)),
        out_shape=jax.ShapeDtypeStruct((n_heads, dim + 8, n_glob), F32),
        grid=(n_heads,),
        in_specs=[head((n_glob, dim)), head((n_rows, dim)), head((n_rows, dim))],
        out_specs=head((dim + 8, n_glob)),
        cost_estimate=pl.CostEstimate(flops=8 * work * dim, bytes_accessed=24 << 20, transcendentals=work),
        compiler_params=pltpu.CompilerParams(dimension_semantics=("arbitrary",), vmem_limit_bytes=62 << 20),
        name="global_queries",
    )(q_glob, k, v)


def merge_parts(parts, dim):
    tops = [p[:, dim:dim + 1, :] for p in parts]
    top = functools.reduce(jnp.maximum, tops)
    weights = [p[:, dim + 1:dim + 2, :] * jnp.exp2(t - top) for p, t in zip(parts, tops)]
    inv = 1.0 / functools.reduce(jnp.add, weights)
    return functools.reduce(jnp.add, [p[:, :dim, :] * (w * inv) for p, w in zip(parts, weights)]).astype(BF16)


def hidden_kernel(where_ref, gpos_ref, om_ref, oo_ref, gm_ref, go_ref, x_ref, wm_ref, w0_ref, w1_ref, h_ref, mine, other):
    size = x_ref.shape[0]
    n_parts, _, part = other.shape

    @pl.when(pl.program_id(0) == 0)
    def _():
        row = where_ref[1] + lax.broadcasted_iota(jnp.int32, (size, gpos_ref.shape[1]), 0)
        hit = jnp.where(row == gpos_ref[...], 1.0, 0.0)
        is_glob = jnp.max(hit, axis=1, keepdims=True) > 0.0
        pick = hit.astype(BF16)
        for i in range(n_parts):
            cols = slice(i * part, (i + 1) * part)
            rows = contract_last(pick, gm_ref[0, cols, :])
            mine[:, cols] = jnp.where(is_glob, rows, om_ref[:, cols].astype(F32)).astype(BF16)
            rows = contract_last(pick, go_ref[0, cols, :])
            other[i] = jnp.where(is_glob, rows, oo_ref[:, cols].astype(F32)).astype(BF16)

    a_mine = jnp.dot(mine[...], wm_ref[...], preferred_element_type=F32)
    a_other = jnp.dot(other[where_ref[2]], w0_ref[...], preferred_element_type=F32)
    a_other = a_other + jnp.dot(other[where_ref[3]], w1_ref[...], preferred_element_type=F32)
    h_ref[...] = (x_ref[...].astype(F32) + (a_mine + a_other)).astype(BF16)


def hidden_block(where, gpos, o_mine, o_other, glob, x, wo_mine, wo_parts, local, size):
    heads, width = wo_mine.shape
    n_glob = gpos.shape[1]
    tile = 512
    n_parts = len(wo_parts)
    part = heads // n_parts
    return pl.pallas_call(
        hidden_kernel,
        out_shape=jax.ShapeDtypeStruct((size, width), BF16),
        grid_spec=pltpu.PrefetchScalarGridSpec(
            num_scalar_prefetch=1,
            grid=(width // tile,),
            in_specs=[
                pl.BlockSpec((1, n_glob), lambda j, r: (0, 0)),
                pl.BlockSpec((size, heads), lambda j, r: (local, 0)),
                pl.BlockSpec((size, heads), lambda j, r: (local, 0)),
                pl.BlockSpec((1, heads, n_glob), lambda j, r: (0, 0, 0)),
                pl.BlockSpec((1, heads, n_glob), lambda j, r: (1, 0, 0)),
                pl.BlockSpec((size, tile), lambda j, r: (r[0], j)),
                pl.BlockSpec((heads, tile), lambda j, r: (0, j)),
            ] + [pl.BlockSpec((part, tile), lambda j, r: (0, j))] * n_parts,
            out_specs=pl.BlockSpec((size, tile), lambda j, r: (0, j)),
            scratch_shapes=[pltpu.VMEM((size, heads), BF16), pltpu.VMEM((n_parts, size, part), BF16)],
        ),
        cost_estimate=pl.CostEstimate(flops=4 * size * heads * (width + n_glob), bytes_accessed=40 << 20, transcendentals=0),
        compiler_params=pltpu.CompilerParams(dimension_semantics=("arbitrary",), vmem_limit_bytes=62 << 20),
        name="hidden_rows",
    )(where, gpos, o_mine, o_other, glob, glob, x, wo_mine, *wo_parts)


def gate(value, *deps):
    return lax.optimization_barrier((value,) + deps)[0]


def solution(mesh):
    n_seq = mesh.shape['sp']
    to_right = [(i, i + 1) for i in range(n_seq - 1)]
    to_left = [(i + 1, i) for i in range(n_seq - 1)]
    swap = [(0, 1), (1, 0)]
    swap_core = [(i, i ^ 1) for i in range(n_seq)]
    swap_chip = [(i, i ^ 2) for i in range(n_seq)]

    def device_layer(tokens, glob_pos, w_query, w_key, w_value, w_out, w_up, w_down):
        n_rows, width = tokens.shape
        n_heads, dim = w_query.shape[1:]
        n_glob = glob_pos.shape[0]
        seq_len = n_rows * n_seq
        sp, tp = lax.axis_index('sp'), lax.axis_index('tp')
        first_row = sp * n_rows
        heads = n_heads * dim
        half = n_rows // 2
        away, home = (1 - tp) * half, tp * half
        quarters = [sp, sp ^ 2, sp ^ 1, sp ^ 3]

        row_ids = first_row + jnp.arange(n_rows)
        pick = (glob_pos[:, None] == row_ids[None, :]).astype(BF16)
        picked = jnp.dot(pick, tokens, preferred_element_type=F32).astype(BF16)
        chip_sum = picked + lax.ppermute(picked, 'sp', swap_core)
        core = sp % 2
        side = lax.dynamic_slice_in_dim(chip_sum, core * (width // 2), width // 2, axis=1)
        side = side + lax.ppermute(side, 'sp', swap_chip)
        side_other = lax.ppermute(side, 'sp', swap_core)
        x_glob = jnp.where(core == 0, jnp.concatenate([side, side_other], axis=1),
                           jnp.concatenate([side_other, side], axis=1))

        wo_mine = w_out.reshape(heads, width)
        part = heads // 2
        wo_0 = lax.ppermute(lax.dynamic_slice_in_dim(wo_mine, core * part, part), 'tp', swap)
        wo_parts = (wo_0, lax.ppermute(wo_0, 'sp', swap_core))

        key_pos = first_row - WIN + jnp.arange(n_rows + 2 * WIN)
        key_glob = jnp.any(key_pos[:, None] == glob_pos[None, :], axis=1)
        key_ok = (key_pos >= 0) & (key_pos < seq_len) & jnp.logical_not(key_glob)
        bias = jnp.broadcast_to(jnp.where(key_ok, 0.0, -jnp.inf)[:, None], (n_rows + 2 * WIN, 128)).astype(F32)

        def project(rows, weight):
            return jnp.einsum('rd,dhe->hre', rows, weight, preferred_element_type=F32).astype(BF16)

        k_rows = project(gate(tokens, picked, bias), w_key)
        left_k = lax.ppermute(k_rows[:, n_rows - WIN:], 'sp', to_right)
        right_k = lax.ppermute(k_rows[:, :WIN], 'sp', to_left)
        v_rows = project(gate(tokens, k_rows), w_value)
        left_v = lax.ppermute(v_rows[:, n_rows - WIN:], 'sp', to_right)
        right_v = lax.ppermute(v_rows[:, :WIN], 'sp', to_left)
        q_rows = project(gate(tokens, v_rows), w_query)
        x_glob = gate(x_glob, q_rows)

        q_glob = project(x_glob, w_query)
        mine = glob_part(q_glob, k_rows, v_rows)
        share = n_glob // n_seq
        parts = [lax.dynamic_slice_in_dim(mine, sp * share, share, axis=2)]
        for step in range(1, n_seq):
            dest = lax.rem(sp + step, n_seq)
            piece = lax.dynamic_slice_in_dim(mine, dest * share, share, axis=2)
            parts.append(lax.ppermute(piece, 'sp', [(i, (i + step) % n_seq) for i in range(n_seq)]))
        k_glob = project(gate(x_glob, mine), w_key)
        v_glob = project(gate(x_glob, k_glob), w_value)

        def window(start, *deps):
            row = gate(start.reshape(1), *deps)
            return window_rows(row, q_rows, k_rows, v_rows, left_k, left_v, right_k, right_v, k_glob, v_glob, bias)

        att, att_other = {}, {}
        att['h0'] = window(home)
        merged = merge_parts([gate(parts[0], att['h0'])] + parts[1:], dim).reshape(heads, share)
        merged_other = lax.ppermute(merged, 'tp', swap)
        att_other['a0'] = lax.ppermute(gate(att['h0'], merged), 'tp', swap)
        att['h1'] = window(home + ROWS, merged)
        att_other['a1'] = lax.ppermute(att['h1'], 'tp', swap)
        glob = jnp.stack([merged, gate(merged_other, att['h1'])])
        glob = jnp.concatenate([glob, lax.ppermute(glob, 'sp', swap_chip)], axis=2)
        att['a0'] = window(away, att['h1'])
        att_other['h0'] = lax.ppermute(att['a0'], 'tp', swap)
        glob = gate(glob, att['a0'])
        glob = jnp.concatenate([glob, lax.ppermute(glob, 'sp', swap_core)], axis=2)
        gpos = jnp.concatenate([lax.dynamic_slice_in_dim(glob_pos, q * share, share) for q in quarters]).reshape(1, n_glob)

        def hidden_rows(key, start, offset, size, dep):
            row = start + offset
            where = jnp.stack([row // size, first_row + row, core, 1 - core]).astype(jnp.int32)
            return hidden_block(gate(where, dep), gpos, att[key], att_other[key], glob, tokens, wo_mine, wo_parts,
                                (offset % ROWS) // size, size)

        def mlp(h_blk):
            u = jax.nn.gelu(jnp.dot(h_blk, w_up, preferred_element_type=F32), approximate=True).astype(BF16)
            return lax.optimization_barrier(jnp.dot(u, w_down, preferred_element_type=F32))

        sums, dep = [], att['a0']
        for i, (key, offset, size) in enumerate((('a0', 0, 256), ('a0', 256, 256), ('a1', 512, 512))):
            dep = partial = mlp(hidden_rows(key, away, offset, size, dep))
            sums.append(lax.ppermute(partial, 'tp', swap))
            if i == 0:
                dep = att['a1'] = window(away + ROWS, partial)
                att_other['h1'] = lax.ppermute(att['a1'], 'tp', swap)

        def finish(h_blk, partial, total):
            return lax.optimization_barrier((h_blk.astype(F32) + (partial + total)).astype(BF16))

        pieces, y_other = [], []
        for c, arrived in ((0, sums[:2]), (1, sums[2:])):
            h_blk = hidden_rows('h%d' % c, home, c * ROWS, ROWS, dep)
            dep = partial = mlp(h_blk)
            size = ROWS // len(arrived)
            for i, total in enumerate(arrived):
                y = finish(h_blk[i * size:(i + 1) * size], partial[i * size:(i + 1) * size], gate(total, partial))
                y_other.append(lax.ppermute(y, 'tp', swap))
                pieces.append((y, c * ROWS + i * size))
        out = gate(jnp.zeros((n_rows, width), BF16), dep)
        for y, offset in pieces:
            out = lax.dynamic_update_slice_in_dim(out, y, home + offset, 0)
        for y, (_, offset) in zip(y_other, pieces):
            out = lax.dynamic_update_slice_in_dim(gate(out, pieces[-1][0]), y, away + offset, 0)
        return out

    row_spec = P(('dp', 'sp'), None)
    head_spec = P(None, 'tp', None)
    in_specs = (row_spec, P('dp'), head_spec, head_spec, head_spec, P('tp', None, None), P(None, 'tp'), P('tp', None))
    return jax.shard_map(device_layer, mesh=mesh, in_specs=in_specs, out_specs=row_spec, check_vma=False)
```

```python
import functools
import math

import jax
import jax.numpy as jnp
from jax import lax
from jax.experimental import pallas as pl
from jax.experimental.pallas import tpu as pltpu
from jax.sharding import PartitionSpec as P


WIN = 256
QB = 256
STEP_HEADS = 4
MLP_TILE = 1024
ROWS = 512
F32 = jnp.float32
BF16 = jnp.bfloat16
LOG2E = 1.4426950408889634


def contract_last(a, b):
    return lax.dot_general(a, b, (((1,), (1,)), ((), ())), preferred_element_type=F32)


def contract_first(a, b):
    return lax.dot_general(a, b, (((0,), (0,)), ((), ())), preferred_element_type=F32)


def window_kernel(r0_ref, q_ref, k_ref, v_ref, lk_ref, lv_ref, rk_ref, rv_ref, *refs, coef):
    *globs, bias_ref, o_ref, k_win, v_win, k_all, v_all, mask = refs
    n_globs = len(globs) // 2
    n_rows = k_ref.shape[1]
    r0 = pl.multiple_of(r0_ref[0], ROWS)

    @pl.when(pl.program_id(0) == 0)
    def _():
        key = lax.broadcasted_iota(jnp.int32, (QB + 2 * WIN, QB), 0)
        query = lax.broadcasted_iota(jnp.int32, (QB + 2 * WIN, QB), 1)
        band = (key >= query) & (key <= query + 2 * WIN)
        for b in range(ROWS // QB):
            rows = bias_ref[pl.ds(pl.multiple_of(r0 + b * QB, QB), QB + 2 * WIN), :]
            mask[b] = jnp.where(band, jnp.concatenate([rows] * (QB // 128), axis=1), -jnp.inf)

    before = pl.multiple_of(jnp.maximum(r0 - WIN, 0), WIN)
    after = pl.multiple_of(jnp.minimum(r0 + ROWS, n_rows - WIN), WIN)
    n_heads = k_ref.shape[0]
    for h in range(n_heads):
        for src, left, right, dst in ((k_ref, lk_ref, rk_ref, k_win), (v_ref, lv_ref, rv_ref, v_win)):
            dst[h, 0:WIN, :] = jnp.where(r0 == 0, left[0, h], src[h, pl.ds(before, WIN), :])
            dst[h, WIN:WIN + ROWS, :] = src[h, pl.ds(r0, ROWS), :]
            dst[h, WIN + ROWS:, :] = jnp.where(r0 + ROWS == n_rows, right[0, h], src[h, pl.ds(after, WIN), :])
        for dst, parts in ((k_all, globs[:n_globs]), (v_all, globs[n_globs:])):
            for i, part in enumerate(parts):
                size = part.shape[2]
                dst[h, i * size:(i + 1) * size, :] = part[0, h]

    def scores(h, b):
        q_blk = q_ref[h, b * QB:(b + 1) * QB, :]
        s_win = contract_last(k_win[h, b * QB:(b + 1) * QB + 2 * WIN, :], q_blk) * coef + mask[b]
        return s_win, contract_last(k_all[h], q_blk) * coef

    blocks = [(h, b) for h in range(n_heads) for b in range(ROWS // QB)]
    dim = k_ref.shape[2]
    s_win, s_glob = scores(*blocks[0])
    for i, (h, b) in enumerate(blocks):
        following = scores(*blocks[i + 1]) if i + 1 < len(blocks) else (None, None)
        top = jnp.maximum(jnp.max(s_win, axis=0, keepdims=True), jnp.max(s_glob, axis=0, keepdims=True))
        e_win = jnp.exp2(s_win - top)
        e_glob = jnp.exp2(s_glob - top)
        inv = 1.0 / (jnp.sum(e_win, axis=0, keepdims=True) + jnp.sum(e_glob, axis=0, keepdims=True))
        out = contract_first(v_win[h, b * QB:(b + 1) * QB + 2 * WIN, :], (e_win * inv).astype(BF16))
        out = out + contract_first(v_all[h], (e_glob * inv).astype(BF16))
        o_ref[b * QB:(b + 1) * QB, h * dim:(h + 1) * dim] = out.T.astype(BF16)
        s_win, s_glob = following


def window_rows(r0, q, q_block, k, v, left, right, globs, bias):
    n_heads, n_rows, dim = k.shape
    share = globs[0].shape[2]
    n_glob = share * len(globs)

    def head(shape):
        return pl.BlockSpec((STEP_HEADS,) + shape, lambda h, r: (h, 0, 0))

    def item(i, size):
        return pl.BlockSpec((1, STEP_HEADS, size, dim), lambda h, r: (i, h, 0, 0))

    span = ROWS + 2 * WIN
    work = n_heads * ROWS * (QB + 2 * WIN + n_glob)
    return pl.pallas_call(
        functools.partial(window_kernel, coef=LOG2E / math.sqrt(dim)),
        out_shape=jax.ShapeDtypeStruct((ROWS, n_heads * dim), BF16),
        grid_spec=pltpu.PrefetchScalarGridSpec(
            num_scalar_prefetch=1,
            grid=(n_heads // STEP_HEADS,),
            in_specs=[
                pl.BlockSpec((STEP_HEADS, ROWS, dim), lambda h, r: (h, q_block, 0)),
                head((n_rows, dim)), head((n_rows, dim)),
                item(0, WIN), item(1, WIN), item(0, WIN), item(1, WIN),
                *[item(0, share) for _ in globs], *[item(1, share) for _ in globs],
                pl.BlockSpec(bias.shape, lambda h, r: (0, 0)),
            ],
            out_specs=pl.BlockSpec((ROWS, STEP_HEADS * dim), lambda h, r: (0, h)),
            scratch_shapes=[
                pltpu.VMEM((STEP_HEADS, span, dim), BF16),
                pltpu.VMEM((STEP_HEADS, span, dim), BF16),
                pltpu.VMEM((STEP_HEADS, n_glob, dim), BF16),
                pltpu.VMEM((STEP_HEADS, n_glob, dim), BF16),
                pltpu.VMEM((ROWS // QB, QB + 2 * WIN, QB), F32),
            ],
        ),
        cost_estimate=pl.CostEstimate(flops=8 * work * dim, bytes_accessed=28 << 20, transcendentals=work),
        compiler_params=pltpu.CompilerParams(dimension_semantics=("arbitrary",), vmem_limit_bytes=62 << 20),
        name="window_attention",
    )(r0, q, k, v, left, left, right, right, *globs, *globs, bias)


def glob_kernel(*refs, coef):
    n = (len(refs) - 2) // 2
    q_refs, (k_ref, v_ref), o_refs = refs[:n], refs[n:n + 2], refs[n + 2:]
    share, dim = q_refs[0].shape[2:]
    pair = QB // share

    def scores(h, b):
        q_blk = jnp.concatenate([q[0, h] for q in q_refs[b * pair:(b + 1) * pair]], axis=0)
        return contract_last(k_ref[h], q_blk) * coef

    blocks = [(h, b) for h in range(k_ref.shape[0]) for b in range(n // pair)]
    s = scores(*blocks[0])
    for j, (h, b) in enumerate(blocks):
        following = scores(*blocks[j + 1]) if j + 1 < len(blocks) else None
        top = jnp.max(s, axis=0, keepdims=True)
        e = jnp.exp2(s - top)
        total = jnp.sum(e, axis=0, keepdims=True)
        out = contract_first(v_ref[h], (e * (1.0 / total)).astype(BF16))
        row = lax.broadcasted_iota(jnp.int32, (8, QB), 0)
        stats = jnp.where(row == 0, top, total)
        for i in range(pair):
            o_refs[b * pair + i][h, 0:dim, :] = out[:, i * share:(i + 1) * share]
            o_refs[b * pair + i][h, dim:, :] = stats[:, i * share:(i + 1) * share]
        s = following


def glob_part(globs, k, v):
    n_heads, n_rows, dim = k.shape
    share = globs[0].shape[2]
    work = n_heads * n_rows * share * len(globs)

    def head(shape):
        return pl.BlockSpec((STEP_HEADS,) + shape, lambda h: (h, 0, 0))

    return pl.pallas_call(
        functools.partial(glob_kernel, coef=LOG2E / math.sqrt(dim)),
        out_shape=[jax.ShapeDtypeStruct((n_heads, dim + 8, share), F32)] * len(globs),
        grid=(n_heads // STEP_HEADS,),
        in_specs=[pl.BlockSpec((1, STEP_HEADS, share, dim), lambda h: (2, h, 0, 0))] * len(globs) + [head((n_rows, dim))] * 2,
        out_specs=[head((dim + 8, share))] * len(globs),
        cost_estimate=pl.CostEstimate(flops=8 * work * dim, bytes_accessed=24 << 20, transcendentals=work),
        compiler_params=pltpu.CompilerParams(dimension_semantics=("arbitrary",), vmem_limit_bytes=62 << 20),
        name="global_queries",
    )(*globs, k, v)


def merge_parts(parts, dim):
    tops = [p[:, dim:dim + 1, :] for p in parts]
    top = functools.reduce(jnp.maximum, tops)
    weights = [p[:, dim + 1:dim + 2, :] * jnp.exp2(t - top) for p, t in zip(parts, tops)]
    inv = 1.0 / functools.reduce(jnp.add, weights)
    return functools.reduce(jnp.add, [p[:, :dim, :] * (w * inv) for p, w in zip(parts, weights)]).astype(BF16)


def hidden_kernel(where_ref, gpos_ref, om_ref, oo_ref, *refs):
    *globs, x_ref, wm_ref, w0_ref, w1_ref, h_ref, mine, other = refs
    size = x_ref.shape[0]
    n_parts, _, part = other.shape
    n_globs = len(globs) // 2

    @pl.when(pl.program_id(0) == 0)
    def _():
        row = where_ref[1] + lax.broadcasted_iota(jnp.int32, (size, gpos_ref.shape[1]), 0)
        hit = jnp.where(row == gpos_ref[...], 1.0, 0.0)
        is_glob = jnp.max(hit, axis=1, keepdims=True) > 0.0
        pick = hit.astype(BF16)

        def fixed(o_ref, parts, cols):
            rows = contract_last(pick, jnp.concatenate([g[0, cols, :] for g in parts], axis=1))
            return jnp.where(is_glob, rows, o_ref[:, cols].astype(F32)).astype(BF16)

        for i in range(n_parts):
            cols = slice(i * part, (i + 1) * part)
            mine[:, cols] = fixed(om_ref, globs[:n_globs], cols)
            other[i] = fixed(oo_ref, globs[n_globs:], cols)

    a_mine = jnp.dot(mine[...], wm_ref[...], preferred_element_type=F32)
    a_other = jnp.dot(other[where_ref[2]], w0_ref[...], preferred_element_type=F32)
    a_other = a_other + jnp.dot(other[where_ref[3]], w1_ref[...], preferred_element_type=F32)
    h_ref[...] = (x_ref[...].astype(F32) + (a_mine + a_other)).astype(BF16)


def hidden_block(where, gpos, o_mine, o_other, globs, x, wo_mine, wo_parts, local, size):
    heads, width = wo_mine.shape
    n_glob = gpos.shape[1]
    tile = 512
    n_parts = len(wo_parts)
    part = heads // n_parts
    return pl.pallas_call(
        hidden_kernel,
        out_shape=jax.ShapeDtypeStruct((size, width), BF16),
        grid_spec=pltpu.PrefetchScalarGridSpec(
            num_scalar_prefetch=1,
            grid=(width // tile,),
            in_specs=[
                pl.BlockSpec((1, n_glob), lambda j, r: (0, 0)),
                pl.BlockSpec((size, heads), lambda j, r: (local, 0)),
                pl.BlockSpec((size, heads), lambda j, r: (local, 0)),
                *[pl.BlockSpec((1, heads, n_glob // len(globs)), lambda j, r: (0, 0, 0))] * len(globs),
                *[pl.BlockSpec((1, heads, n_glob // len(globs)), lambda j, r: (1, 0, 0))] * len(globs),
                pl.BlockSpec((size, tile), lambda j, r: (r[0], j)),
                pl.BlockSpec((heads, tile), lambda j, r: (0, j)),
            ] + [pl.BlockSpec((part, tile), lambda j, r: (0, j))] * n_parts,
            out_specs=pl.BlockSpec((size, tile), lambda j, r: (0, j)),
            scratch_shapes=[pltpu.VMEM((size, heads), BF16), pltpu.VMEM((n_parts, size, part), BF16)],
        ),
        cost_estimate=pl.CostEstimate(flops=4 * size * heads * (width + n_glob), bytes_accessed=40 << 20, transcendentals=0),
        compiler_params=pltpu.CompilerParams(dimension_semantics=("arbitrary",), vmem_limit_bytes=62 << 20),
        name="hidden_rows",
    )(where, gpos, o_mine, o_other, *globs, *globs, x, wo_mine, *wo_parts)


def mlp_kernel(h_ref, up_ref, down_ref, o_ref):
    z = jnp.dot(h_ref[...], up_ref[...], preferred_element_type=F32)
    u = (0.5 * z * (1.0 + jnp.tanh(math.sqrt(2.0 / math.pi) * (z + 0.044715 * (z * z * z))))).astype(BF16)
    step = pl.program_id(0)

    @pl.when(step == 0)
    def _():
        o_ref[...] = jnp.dot(u, down_ref[...], preferred_element_type=F32)

    @pl.when(step > 0)
    def _():
        o_ref[...] += jnp.dot(u, down_ref[...], preferred_element_type=F32)


def mlp_block(h, w_up, w_down):
    size, width = h.shape
    inner = w_up.shape[1]
    tile = MLP_TILE
    return pl.pallas_call(
        mlp_kernel,
        out_shape=jax.ShapeDtypeStruct((size, width), F32),
        grid=(inner // tile,),
        in_specs=[
            pl.BlockSpec((size, width), lambda j: (0, 0)),
            pl.BlockSpec((width, tile), lambda j: (0, j)),
            pl.BlockSpec((tile, width), lambda j: (j, 0)),
        ],
        out_specs=pl.BlockSpec((size, width), lambda j: (0, 0)),
        cost_estimate=pl.CostEstimate(flops=4 * size * width * inner, bytes_accessed=4 * width * inner, transcendentals=size * inner),
        compiler_params=pltpu.CompilerParams(dimension_semantics=("arbitrary",), vmem_limit_bytes=62 << 20),
        name="mlp_rows",
    )(h, w_up, w_down)


def gate(value, *deps):
    return lax.optimization_barrier((value,) + deps)[0]


def solution(mesh):
    n_seq = mesh.shape['sp']
    to_right = [(i, i + 1) for i in range(n_seq - 1)]
    to_left = [(i + 1, i) for i in range(n_seq - 1)]
    swap = [(0, 1), (1, 0)]
    swap_core = [(i, i ^ 1) for i in range(n_seq)]
    swap_chip = [(i, i ^ 2) for i in range(n_seq)]

    def device_layer(tokens, glob_pos, w_query, w_key, w_value, w_out, w_up, w_down):
        n_rows, width = tokens.shape
        n_heads, dim = w_query.shape[1:]
        n_glob = glob_pos.shape[0]
        seq_len = n_rows * n_seq
        sp, tp = lax.axis_index('sp'), lax.axis_index('tp')
        first_row = sp * n_rows
        heads = n_heads * dim
        half = n_rows // 2
        away, home = (1 - tp) * half, tp * half
        quarters = [sp, sp ^ 2, sp ^ 1, sp ^ 3]

        share = n_glob // n_seq
        gpos = jnp.concatenate([lax.dynamic_slice_in_dim(glob_pos, q * share, share) for q in quarters])

        row_ids = first_row + jnp.arange(n_rows)
        pick = (gpos[:, None] == row_ids[None, :]).astype(BF16)
        picked = jnp.dot(pick, tokens, preferred_element_type=F32).astype(BF16)
        core = sp % 2
        chip_sum = picked[:2 * share] + lax.ppermute(picked[2 * share:], 'sp', swap_core)
        x_glob = chip_sum[:share] + lax.ppermute(chip_sum[share:], 'sp', swap_chip)

        wo_mine = w_out.reshape(heads, width)
        part = heads // 2
        wo_0 = lax.ppermute(lax.dynamic_slice_in_dim(wo_mine, core * part, part), 'tp', swap)
        wo_parts = (wo_0, lax.ppermute(wo_0, 'sp', swap_core))

        key_pos = first_row - WIN + jnp.arange(n_rows + 2 * WIN)
        key_glob = jnp.any(key_pos[:, None] == glob_pos[None, :], axis=1)
        key_ok = (key_pos >= 0) & (key_pos < seq_len) & jnp.logical_not(key_glob)
        bias = jnp.broadcast_to(jnp.where(key_ok, 0.0, -jnp.inf)[:, None], (n_rows + 2 * WIN, 128)).astype(F32)

        def project(rows, weight):
            return jnp.einsum('rd,dhe->hre', rows, weight, preferred_element_type=F32).astype(BF16)

        k_rows = project(gate(tokens, picked, bias), w_key)
        x_glob = gate(x_glob, k_rows)
        of_glob = jnp.stack([project(x_glob, w) for w in (w_key, w_value, w_query)])
        of_chip = lax.ppermute(of_glob, 'sp', swap_chip)
        of_core = lax.ppermute(of_glob, 'sp', swap_core)
        v_rows = project(gate(tokens, of_glob), w_value)
        left = lax.ppermute(jnp.stack([rows[:, n_rows - WIN:] for rows in (k_rows, v_rows)]), 'sp', to_right)
        right = lax.ppermute(jnp.stack([rows[:, :WIN] for rows in (k_rows, v_rows)]), 'sp', to_left)
        of_chip = gate(of_chip, v_rows)
        of_both = lax.ppermute(of_chip, 'sp', swap_core)
        of_globs = [of_glob, of_chip, of_core, of_both]

        def query_rows(start, *deps):
            return project(lax.dynamic_slice_in_dim(tokens, gate(start, *deps), half), w_query)

        q_home = query_rows(home, v_rows, of_chip)

        def window(start, q, block, *deps):
            row = gate((start + block * ROWS).reshape(1), *deps)
            return window_rows(row, q, block, k_rows, v_rows, left, right, of_globs, bias)

        att, att_other = {}, {}
        att['h0'] = window(home, q_home, 0)
        att_other['a0'] = lax.ppermute(att['h0'], 'tp', swap)

        mine = glob_part(of_globs[:1] + [gate(of_chip, att['h0'])] + of_globs[2:], k_rows, v_rows)
        parts = [mine[0]]
        for i in range(1, n_seq):
            flip = (0, 2, 1, 3)[i]
            parts.append(lax.ppermute(mine[i], 'sp', [(j, j ^ flip) for j in range(n_seq)]))
        att['h1'] = window(home, q_home, 1, mine[0])
        att_other['a1'] = lax.ppermute(att['h1'], 'tp', swap)
        q_away = query_rows(away, att['h1'])
        merged = merge_parts([gate(parts[0], q_away)] + parts[1:], dim).reshape(heads, share)
        merged_other = lax.ppermute(merged, 'tp', swap)
        att['a0'] = window(away, q_away, 0, merged)
        att_other['h0'] = lax.ppermute(att['a0'], 'tp', swap)
        glob = jnp.stack([merged, gate(merged_other, att['a0'])])
        glob_chip = lax.ppermute(glob, 'sp', swap_chip)
        glob_core = lax.ppermute(glob, 'sp', swap_core)
        att['a1'] = window(away, q_away, 1, att['a0'])
        att_other['h1'] = lax.ppermute(att['a1'], 'tp', swap)
        glob_chip = gate(glob_chip, att['a1'])
        globs = [glob, glob_chip, glob_core, lax.ppermute(glob_chip, 'sp', swap_core)]
        gpos = gpos.reshape(1, n_glob)

        def hidden_rows(key, start, offset, size, dep):
            row = start + offset
            where = jnp.stack([row // size, first_row + row, core, 1 - core]).astype(jnp.int32)
            return hidden_block(gate(where, dep), gpos, att[key], att_other[key], globs, tokens, wo_mine, wo_parts,
                                (offset % ROWS) // size, size)

        def mlp(h_blk):
            if h_blk.shape[0] < ROWS:
                return mlp_block(h_blk, w_up, w_down)
            u = jax.nn.gelu(jnp.dot(h_blk, w_up, preferred_element_type=F32), approximate=True).astype(BF16)
            return lax.optimization_barrier(jnp.dot(u, w_down, preferred_element_type=F32))

        sums, dep = [], att['a1']
        for key, offset, size in (('a0', 0, 256), ('a0', 256, 256), ('a1', 512, 512)):
            dep = partial = mlp(hidden_rows(key, away, offset, size, dep))
            sums.append(lax.ppermute(partial, 'tp', swap))

        def finish(h_blk, partial, total):
            return lax.optimization_barrier((h_blk.astype(F32) + (partial + total)).astype(BF16))

        pieces, y_other = [], []
        for c, arrived in ((0, sums[:2]), (1, [sums[2][:256], sums[2][256:]])):
            h_blk = hidden_rows('h%d' % c, home, c * ROWS, ROWS, dep)
            dep = partial = mlp(h_blk)
            size = ROWS // len(arrived)
            for i, total in enumerate(arrived):
                y = finish(h_blk[i * size:(i + 1) * size], partial[i * size:(i + 1) * size], gate(total, partial))
                y_other.append(lax.ppermute(y, 'tp', swap))
                pieces.append((y, c * ROWS + i * size))
        out = gate(jnp.zeros((n_rows, width), BF16), dep)
        for y, offset in pieces:
            out = lax.dynamic_update_slice_in_dim(out, y, home + offset, 0)
        for y, (_, offset) in zip(y_other, pieces):
            out = lax.dynamic_update_slice_in_dim(gate(out, pieces[-1][0]), y, away + offset, 0)
        return out

    row_spec = P(('dp', 'sp'), None)
    head_spec = P(None, 'tp', None)
    in_specs = (row_spec, P('dp'), head_spec, head_spec, head_spec, P('tp', None, None), P(None, 'tp'), P('tp', None))
    return jax.shard_map(device_layer, mesh=mesh, in_specs=in_specs, out_specs=row_spec, check_vma=False)
```

```python
import functools
import math

import jax
import jax.numpy as jnp
from jax import lax
from jax.experimental import pallas as pl
from jax.experimental.pallas import tpu as pltpu
from jax.sharding import PartitionSpec as P


WIN = 256
QB = 256
STEP_HEADS = 4
MLP_TILE = 1024
ROWS = 512
F32 = jnp.float32
BF16 = jnp.bfloat16
LOG2E = 1.4426950408889634


def contract_last(a, b):
    return lax.dot_general(a, b, (((1,), (1,)), ((), ())), preferred_element_type=F32)


def contract_first(a, b):
    return lax.dot_general(a, b, (((0,), (0,)), ((), ())), preferred_element_type=F32)


def window_kernel(r0_ref, q_ref, k_ref, v_ref, lk_ref, lv_ref, rk_ref, rv_ref, *refs, coef):
    *globs, bias_ref, o_ref, k_win, v_win, k_all, v_all, mask = refs
    n_globs = len(globs) // 2
    n_rows = k_ref.shape[1]
    r0 = pl.multiple_of(r0_ref[0], ROWS)

    @pl.when(pl.program_id(0) == 0)
    def _():
        key = lax.broadcasted_iota(jnp.int32, (QB + 2 * WIN, QB), 0)
        query = lax.broadcasted_iota(jnp.int32, (QB + 2 * WIN, QB), 1)
        band = (key >= query) & (key <= query + 2 * WIN)
        for b in range(ROWS // QB):
            rows = bias_ref[pl.ds(pl.multiple_of(r0 + b * QB, QB), QB + 2 * WIN), :]
            mask[b] = jnp.where(band, jnp.concatenate([rows] * (QB // 128), axis=1), -jnp.inf)

    before = pl.multiple_of(jnp.maximum(r0 - WIN, 0), WIN)
    after = pl.multiple_of(jnp.minimum(r0 + ROWS, n_rows - WIN), WIN)
    n_heads = k_ref.shape[0]
    for h in range(n_heads):
        for src, left, right, dst in ((k_ref, lk_ref, rk_ref, k_win), (v_ref, lv_ref, rv_ref, v_win)):
            dst[h, 0:WIN, :] = jnp.where(r0 == 0, left[0, h], src[h, pl.ds(before, WIN), :])
            dst[h, WIN:WIN + ROWS, :] = src[h, pl.ds(r0, ROWS), :]
            dst[h, WIN + ROWS:, :] = jnp.where(r0 + ROWS == n_rows, right[0, h], src[h, pl.ds(after, WIN), :])
        for dst, parts in ((k_all, globs[:n_globs]), (v_all, globs[n_globs:])):
            for i, part in enumerate(parts):
                size = part.shape[2]
                dst[h, i * size:(i + 1) * size, :] = part[0, h]

    def scores(h, b):
        q_blk = q_ref[h, b * QB:(b + 1) * QB, :]
        s_win = contract_last(k_win[h, b * QB:(b + 1) * QB + 2 * WIN, :], q_blk) * coef + mask[b]
        return s_win, contract_last(k_all[h], q_blk) * coef

    blocks = [(h, b) for h in range(n_heads) for b in range(ROWS // QB)]
    dim = k_ref.shape[2]
    s_win, s_glob = scores(*blocks[0])
    for i, (h, b) in enumerate(blocks):
        following = scores(*blocks[i + 1]) if i + 1 < len(blocks) else (None, None)
        top = jnp.maximum(jnp.max(s_win, axis=0, keepdims=True), jnp.max(s_glob, axis=0, keepdims=True))
        e_win = jnp.exp2(s_win - top)
        e_glob = jnp.exp2(s_glob - top)
        inv = 1.0 / (jnp.sum(e_win, axis=0, keepdims=True) + jnp.sum(e_glob, axis=0, keepdims=True))
        out = contract_first(v_win[h, b * QB:(b + 1) * QB + 2 * WIN, :], (e_win * inv).astype(BF16))
        out = out + contract_first(v_all[h], (e_glob * inv).astype(BF16))
        o_ref[b * QB:(b + 1) * QB, h * dim:(h + 1) * dim] = out.T.astype(BF16)
        s_win, s_glob = following


def window_rows(r0, q, q_block, k, v, left, right, globs, bias):
    n_heads, n_rows, dim = k.shape
    share = globs[0].shape[2]
    n_glob = share * len(globs)

    def head(shape):
        return pl.BlockSpec((STEP_HEADS,) + shape, lambda h, r: (h, 0, 0))

    def item(i, size):
        return pl.BlockSpec((1, STEP_HEADS, size, dim), lambda h, r: (i, h, 0, 0))

    span = ROWS + 2 * WIN
    work = n_heads * ROWS * (QB + 2 * WIN + n_glob)
    return pl.pallas_call(
        functools.partial(window_kernel, coef=LOG2E / math.sqrt(dim)),
        out_shape=jax.ShapeDtypeStruct((ROWS, n_heads * dim), BF16),
        grid_spec=pltpu.PrefetchScalarGridSpec(
            num_scalar_prefetch=1,
            grid=(n_heads // STEP_HEADS,),
            in_specs=[
                pl.BlockSpec((STEP_HEADS, ROWS, dim), lambda h, r: (h, q_block, 0)),
                head((n_rows, dim)), head((n_rows, dim)),
                item(0, WIN), item(1, WIN), item(0, WIN), item(1, WIN),
                *[item(0, share) for _ in globs], *[item(1, share) for _ in globs],
                pl.BlockSpec(bias.shape, lambda h, r: (0, 0)),
            ],
            out_specs=pl.BlockSpec((ROWS, STEP_HEADS * dim), lambda h, r: (0, h)),
            scratch_shapes=[
                pltpu.VMEM((STEP_HEADS, span, dim), BF16),
                pltpu.VMEM((STEP_HEADS, span, dim), BF16),
                pltpu.VMEM((STEP_HEADS, n_glob, dim), BF16),
                pltpu.VMEM((STEP_HEADS, n_glob, dim), BF16),
                pltpu.VMEM((ROWS // QB, QB + 2 * WIN, QB), F32),
            ],
        ),
        cost_estimate=pl.CostEstimate(flops=8 * work * dim, bytes_accessed=28 << 20, transcendentals=work),
        compiler_params=pltpu.CompilerParams(vmem_limit_bytes=62 << 20),
        name="window",
    )(r0, q, k, v, left, left, right, right, *globs, *globs, bias)


def glob_kernel(*refs, coef):
    n = (len(refs) - 2) // 2
    q_refs, (k_ref, v_ref), o_refs = refs[:n], refs[n:n + 2], refs[n + 2:]
    share, dim = q_refs[0].shape[2:]
    pair = QB // share

    def scores(h, b):
        q_blk = jnp.concatenate([q[0, h] for q in q_refs[b * pair:(b + 1) * pair]], axis=0)
        return contract_last(k_ref[h], q_blk) * coef

    blocks = [(h, b) for h in range(k_ref.shape[0]) for b in range(n // pair)]
    s = scores(*blocks[0])
    for j, (h, b) in enumerate(blocks):
        following = scores(*blocks[j + 1]) if j + 1 < len(blocks) else None
        top = jnp.max(s, axis=0, keepdims=True)
        e = jnp.exp2(s - top)
        total = jnp.sum(e, axis=0, keepdims=True)
        out = contract_first(v_ref[h], (e * (1.0 / total)).astype(BF16))
        row = lax.broadcasted_iota(jnp.int32, (8, QB), 0)
        stats = jnp.where(row == 0, top, total)
        for i in range(pair):
            o_refs[b * pair + i][h, 0:dim, :] = out[:, i * share:(i + 1) * share]
            o_refs[b * pair + i][h, dim:, :] = stats[:, i * share:(i + 1) * share]
        s = following


def glob_part(globs, k, v):
    n_heads, n_rows, dim = k.shape
    share = globs[0].shape[2]
    work = n_heads * n_rows * share * len(globs)

    def head(shape):
        return pl.BlockSpec((STEP_HEADS,) + shape, lambda h: (h, 0, 0))

    return pl.pallas_call(
        functools.partial(glob_kernel, coef=LOG2E / math.sqrt(dim)),
        out_shape=[jax.ShapeDtypeStruct((n_heads, dim + 8, share), F32)] * len(globs),
        grid=(n_heads // STEP_HEADS,),
        in_specs=[pl.BlockSpec((1, STEP_HEADS, share, dim), lambda h: (2, h, 0, 0))] * len(globs) + [head((n_rows, dim))] * 2,
        out_specs=[head((dim + 8, share))] * len(globs),
        cost_estimate=pl.CostEstimate(flops=8 * work * dim, bytes_accessed=24 << 20, transcendentals=work),
        compiler_params=pltpu.CompilerParams(vmem_limit_bytes=62 << 20),
        name="globals",
    )(*globs, k, v)


def merge_parts(parts, dim):
    tops = [p[:, dim:dim + 1, :] for p in parts]
    top = functools.reduce(jnp.maximum, tops)
    weights = [p[:, dim + 1:dim + 2, :] * jnp.exp2(t - top) for p, t in zip(parts, tops)]
    inv = 1.0 / functools.reduce(jnp.add, weights)
    return functools.reduce(jnp.add, [p[:, :dim, :] * (w * inv) for p, w in zip(parts, weights)]).astype(BF16)


def hidden_kernel(where_ref, gpos_ref, om_ref, oo_ref, *refs):
    *globs, x_ref, wm_ref, w0_ref, w1_ref, h_ref, mine, other = refs
    size = x_ref.shape[0]
    n_parts, _, part = other.shape
    n_globs = len(globs) // 2

    @pl.when(pl.program_id(0) == 0)
    def _():
        row = where_ref[1] + lax.broadcasted_iota(jnp.int32, (size, gpos_ref.shape[1]), 0)
        hit = jnp.where(row == gpos_ref[...], 1.0, 0.0)
        is_glob = jnp.max(hit, axis=1, keepdims=True) > 0.0
        pick = hit.astype(BF16)

        def fixed(o_ref, parts, cols):
            rows = contract_last(pick, jnp.concatenate([g[0, cols, :] for g in parts], axis=1))
            return jnp.where(is_glob, rows, o_ref[:, cols].astype(F32)).astype(BF16)

        for i in range(n_parts):
            cols = slice(i * part, (i + 1) * part)
            mine[:, cols] = fixed(om_ref, globs[:n_globs], cols)
            other[i] = fixed(oo_ref, globs[n_globs:], cols)

    a_mine = jnp.dot(mine[...], wm_ref[...], preferred_element_type=F32)
    a_other = jnp.dot(other[where_ref[2]], w0_ref[...], preferred_element_type=F32)
    a_other = a_other + jnp.dot(other[where_ref[3]], w1_ref[...], preferred_element_type=F32)
    h_ref[...] = (x_ref[...].astype(F32) + (a_mine + a_other)).astype(BF16)


def hidden_block(where, gpos, o_mine, o_other, globs, x, wo_mine, wo_parts, local, size):
    heads, width = wo_mine.shape
    n_glob = gpos.shape[1]
    tile = 512
    n_parts = len(wo_parts)
    part = heads // n_parts
    return pl.pallas_call(
        hidden_kernel,
        out_shape=jax.ShapeDtypeStruct((size, width), BF16),
        grid_spec=pltpu.PrefetchScalarGridSpec(
            num_scalar_prefetch=1,
            grid=(width // tile,),
            in_specs=[
                pl.BlockSpec((1, n_glob), lambda j, r: (0, 0)),
                pl.BlockSpec((size, heads), lambda j, r: (local, 0)),
                pl.BlockSpec((size, heads), lambda j, r: (local, 0)),
                *[pl.BlockSpec((1, heads, n_glob // len(globs)), lambda j, r: (0, 0, 0))] * len(globs),
                *[pl.BlockSpec((1, heads, n_glob // len(globs)), lambda j, r: (1, 0, 0))] * len(globs),
                pl.BlockSpec((size, tile), lambda j, r: (r[0], j)),
                pl.BlockSpec((heads, tile), lambda j, r: (0, j)),
            ] + [pl.BlockSpec((part, tile), lambda j, r: (0, j))] * n_parts,
            out_specs=pl.BlockSpec((size, tile), lambda j, r: (0, j)),
            scratch_shapes=[pltpu.VMEM((size, heads), BF16), pltpu.VMEM((n_parts, size, part), BF16)],
        ),
        cost_estimate=pl.CostEstimate(flops=4 * size * heads * (width + n_glob), bytes_accessed=40 << 20, transcendentals=0),
        compiler_params=pltpu.CompilerParams(vmem_limit_bytes=62 << 20),
        name="hidden",
    )(where, gpos, o_mine, o_other, *globs, *globs, x, wo_mine, *wo_parts)


def mlp_kernel(h_ref, up_ref, down_ref, o_ref):
    z = jnp.dot(h_ref[...], up_ref[...], preferred_element_type=F32)
    u = (0.5 * z * (1.0 + jnp.tanh(math.sqrt(2.0 / math.pi) * (z + 0.044715 * (z * z * z))))).astype(BF16)
    step = pl.program_id(0)

    @pl.when(step == 0)
    def _():
        o_ref[...] = jnp.dot(u, down_ref[...], preferred_element_type=F32)

    @pl.when(step > 0)
    def _():
        o_ref[...] += jnp.dot(u, down_ref[...], preferred_element_type=F32)


def mlp_block(h, w_up, w_down):
    size, width = h.shape
    inner = w_up.shape[1]
    tile = MLP_TILE
    return pl.pallas_call(
        mlp_kernel,
        out_shape=jax.ShapeDtypeStruct((size, width), F32),
        grid=(inner // tile,),
        in_specs=[
            pl.BlockSpec((size, width), lambda j: (0, 0)),
            pl.BlockSpec((width, tile), lambda j: (0, j)),
            pl.BlockSpec((tile, width), lambda j: (j, 0)),
        ],
        out_specs=pl.BlockSpec((size, width), lambda j: (0, 0)),
        cost_estimate=pl.CostEstimate(flops=4 * size * width * inner, bytes_accessed=4 * width * inner, transcendentals=size * inner),
        compiler_params=pltpu.CompilerParams(vmem_limit_bytes=62 << 20),
        name="mlp",
    )(h, w_up, w_down)


def up_kernel(h_ref, up_ref, u_ref):
    z = jnp.dot(h_ref[...], up_ref[...], preferred_element_type=F32)
    u_ref[...] = (0.5 * z * (1.0 + jnp.tanh(math.sqrt(2.0 / math.pi) * (z + 0.044715 * (z * z * z))))).astype(BF16)


def down_kernel(u_ref, down_ref, o_ref):
    o_ref[...] = jnp.dot(u_ref[...], down_ref[...], preferred_element_type=F32)


def column_call(kernel, rows, weight, start, stop, tile, dtype):
    size, depth = rows.shape
    first = start // tile
    return pl.pallas_call(
        kernel,
        out_shape=jax.ShapeDtypeStruct((size, stop - start), dtype),
        grid=((stop - start) // tile,),
        in_specs=[pl.BlockSpec((size, depth), lambda j: (0, 0)), pl.BlockSpec((depth, tile), lambda j: (0, first + j))],
        out_specs=pl.BlockSpec((size, tile), lambda j: (0, j)),
        cost_estimate=pl.CostEstimate(flops=2 * size * depth * (stop - start), bytes_accessed=2 * depth * (stop - start), transcendentals=0),
        compiler_params=pltpu.CompilerParams(vmem_limit_bytes=62 << 20),
    )(rows, weight)


def gate(value, *deps):
    return lax.optimization_barrier((value,) + deps)[0]


def solution(mesh):
    n_seq = mesh.shape['sp']
    to_right = [(i, i + 1) for i in range(n_seq - 1)]
    to_left = [(i + 1, i) for i in range(n_seq - 1)]
    swap = [(0, 1), (1, 0)]
    swap_core = [(i, i ^ 1) for i in range(n_seq)]
    swap_chip = [(i, i ^ 2) for i in range(n_seq)]

    def device_layer(tokens, glob_pos, w_query, w_key, w_value, w_out, w_up, w_down):
        n_rows, width = tokens.shape
        n_heads, dim = w_query.shape[1:]
        n_glob = glob_pos.shape[0]
        seq_len = n_rows * n_seq
        sp, tp = lax.axis_index('sp'), lax.axis_index('tp')
        first_row = sp * n_rows
        heads = n_heads * dim
        half = n_rows // 2
        away, home = (1 - tp) * half, tp * half
        quarters = [sp, sp ^ 2, sp ^ 1, sp ^ 3]

        share = n_glob // n_seq
        gpos = jnp.concatenate([lax.dynamic_slice_in_dim(glob_pos, q * share, share) for q in quarters])

        row_ids = first_row + jnp.arange(n_rows)
        pick = (gpos[:, None] == row_ids[None, :]).astype(BF16)
        picked = jnp.dot(pick, tokens, preferred_element_type=F32).astype(BF16)
        core = sp % 2
        chip_sum = picked[:2 * share] + lax.ppermute(picked[2 * share:], 'sp', swap_core)
        x_glob = chip_sum[:share] + lax.ppermute(chip_sum[share:], 'sp', swap_chip)

        wo_mine = w_out.reshape(heads, width)
        part = heads // 2
        wo_0 = lax.ppermute(lax.dynamic_slice_in_dim(wo_mine, core * part, part), 'tp', swap)
        wo_parts = (wo_0, lax.ppermute(wo_0, 'sp', swap_core))

        key_pos = first_row - WIN + jnp.arange(n_rows + 2 * WIN)
        key_glob = jnp.any(key_pos[:, None] == glob_pos[None, :], axis=1)
        key_ok = (key_pos >= 0) & (key_pos < seq_len) & jnp.logical_not(key_glob)
        bias = jnp.broadcast_to(jnp.where(key_ok, 0.0, -jnp.inf)[:, None], (n_rows + 2 * WIN, 128)).astype(F32)

        def project(rows, weight):
            return jnp.einsum('rd,dhe->hre', rows, weight, preferred_element_type=F32).astype(BF16)

        k_rows = project(gate(tokens, picked, bias), w_key)
        x_glob = gate(x_glob, k_rows)
        of_glob = jnp.stack([project(x_glob, w) for w in (w_key, w_value, w_query)])
        of_chip = lax.ppermute(of_glob, 'sp', swap_chip)
        of_core = lax.ppermute(of_glob, 'sp', swap_core)
        v_rows = project(gate(tokens, of_glob), w_value)
        left = lax.ppermute(jnp.stack([rows[:, n_rows - WIN:] for rows in (k_rows, v_rows)]), 'sp', to_right)
        right = lax.ppermute(jnp.stack([rows[:, :WIN] for rows in (k_rows, v_rows)]), 'sp', to_left)
        of_chip = gate(of_chip, v_rows)
        of_both = lax.ppermute(of_chip, 'sp', swap_core)
        of_globs = [of_glob, of_chip, of_core, of_both]

        def query_rows(start, *deps):
            return project(lax.dynamic_slice_in_dim(tokens, gate(start, *deps), half), w_query)

        q_home = query_rows(home, v_rows, of_chip)

        def window(start, q, block, *deps):
            row = gate((start + block * ROWS).reshape(1), *deps)
            return window_rows(row, q, block, k_rows, v_rows, left, right, of_globs, bias)

        att, att_other = {}, {}
        att['h0'] = window(home, q_home, 0)
        att_other['a0'] = lax.ppermute(att['h0'], 'tp', swap)

        mine = glob_part(of_globs[:1] + [gate(of_chip, att['h0'])] + of_globs[2:], k_rows, v_rows)
        parts = [mine[0]]
        for i in range(1, n_seq):
            flip = (0, 2, 1, 3)[i]
            parts.append(lax.ppermute(mine[i], 'sp', [(j, j ^ flip) for j in range(n_seq)]))
        att['h1'] = window(home, q_home, 1, mine[0])
        att_other['a1'] = lax.ppermute(att['h1'], 'tp', swap)
        q_away = query_rows(away, att['h1'])
        merged = merge_parts([gate(parts[0], q_away)] + parts[1:], dim).reshape(heads, share)
        merged_other = lax.ppermute(merged, 'tp', swap)
        att['a0'] = window(away, q_away, 0, merged)
        att_other['h0'] = lax.ppermute(att['a0'], 'tp', swap)
        glob = jnp.stack([merged, gate(merged_other, att['a0'])])
        glob_chip = lax.ppermute(glob, 'sp', swap_chip)
        glob_core = lax.ppermute(glob, 'sp', swap_core)
        att['a1'] = window(away, q_away, 1, att['a0'])
        att_other['h1'] = lax.ppermute(att['a1'], 'tp', swap)
        glob_chip = gate(glob_chip, att['a1'])
        globs = [glob, glob_chip, glob_core, lax.ppermute(glob_chip, 'sp', swap_core)]
        gpos = gpos.reshape(1, n_glob)

        def hidden_rows(key, start, offset, size, dep):
            row = start + offset
            where = jnp.stack([row // size, first_row + row, core, 1 - core]).astype(jnp.int32)
            return hidden_block(gate(where, dep), gpos, att[key], att_other[key], globs, tokens, wo_mine, wo_parts,
                                (offset % ROWS) // size, size)

        def mlp(h_blk):
            if h_blk.shape[0] < ROWS:
                return mlp_block(h_blk, w_up, w_down)
            u = jax.nn.gelu(jnp.dot(h_blk, w_up, preferred_element_type=F32), approximate=True).astype(BF16)
            return lax.optimization_barrier(jnp.dot(u, w_down, preferred_element_type=F32))

        h_blk = hidden_rows('a0', away, 0, 256, att['a1'])
        u = column_call(up_kernel, h_blk, w_up, 0, w_up.shape[1], 1024, BF16)
        early = column_call(down_kernel, u, w_down, 0, width // 4, 512, F32)
        dep = late = column_call(down_kernel, gate(u, early), w_down, width // 4, width, 512, F32)
        sums = [(lax.ppermute(early, 'tp', swap), lax.ppermute(late, 'tp', swap))]
        dep = partial = mlp(hidden_rows('a0', away, 256, 256, dep))
        sums.append(lax.ppermute(partial, 'tp', swap))
        h_blk = hidden_rows('a1', away, ROWS, ROWS, dep)
        u = jax.nn.gelu(jnp.dot(h_blk, w_up, preferred_element_type=F32), approximate=True).astype(BF16)
        early = column_call(down_kernel, u, w_down, 0, width // 2, 512, F32)
        dep = late = column_call(down_kernel, gate(u, early), w_down, width // 2, width, 512, F32)
        sums.append((lax.ppermute(early, 'tp', swap), lax.ppermute(late, 'tp', swap)))

        def finish(h_blk, partial, total):
            return lax.optimization_barrier((h_blk.astype(F32) + (partial + total)).astype(BF16))

        pieces, y_other = [], []
        for c in range(2):
            h_blk = hidden_rows('h%d' % c, home, c * ROWS, ROWS, dep)
            dep = partial = mlp(h_blk)
            if c == 0:
                arrived = [jnp.concatenate([gate(p, partial) for p in sums[0]], axis=1), sums[1]]
            else:
                pair = [gate(p, partial) for p in sums[2]]
                arrived = [jnp.concatenate([p[i:i + 256] for p in pair], axis=1) for i in (0, 256)]
            size = ROWS // len(arrived)
            for i, total in enumerate(arrived):
                y = finish(h_blk[i * size:(i + 1) * size], partial[i * size:(i + 1) * size], gate(total, partial))
                y_other.append(lax.ppermute(y, 'tp', swap))
                pieces.append((y, c * ROWS + i * size))
        out = gate(jnp.zeros((n_rows, width), BF16), dep)
        for y, offset in pieces:
            out = lax.dynamic_update_slice_in_dim(out, y, home + offset, 0)
        for y, (_, offset) in zip(y_other, pieces):
            out = lax.dynamic_update_slice_in_dim(gate(out, pieces[-1][0]), y, away + offset, 0)
        return out

    row_spec = P(('dp', 'sp'), None)
    head_spec = P(None, 'tp', None)
    in_specs = (row_spec, P('dp'), head_spec, head_spec, head_spec, P('tp', None, None), P(None, 'tp'), P('tp', None))
    return jax.shard_map(device_layer, mesh=mesh, in_specs=in_specs, out_specs=row_spec, check_vma=False)
```
